32 devices in a mesh: dom: 16 (over z, y, x), feat: 2 (over core).
Axes of the slice: x: 2, y: 2, z: 4, core: 2. Of those that a mesh axis runs over, the one named last changes fastest.
Arguments:
- features: bfloat16 [32768, 608], P('dom', 'feat'), may hold values from -6 to 6
- weight: bfloat16 [608, 256], replicated, may hold values from -0.25 to 0.25
- out_bias: float32 [256], P('feat'), may hold values from -3 to 3
- tile_values: bfloat16 [1728, 128, 128], P('dom'), may hold values from -0.25 to 0.25
- tile_rows: int32 [1728], P('dom'), may hold values from 0 to 15
- tile_cols: int32 [1728], P('dom'), may hold values from 0 to 81, as said below
- tile_count: int32 [16], P('dom'), may hold values from 10 to 108, as said below
- send_rows: int32 [16, 8, 1024], P('dom'), may hold values from 0 to 2047
- hub_ids: int32 [256], replicated, may hold values from 0 to 32767, as said below
Outputs:
- activations: bfloat16 [32768, 256], P('dom', 'feat')
The draws below stay inside these ranges and needn't reach their ends.
Inputs may be any that keep to these rules, and one draw needn't show every extreme that they name: `tile_count`: slots at or past a partition's count are not part of the graph; some partition uses all 108 slots. `tile_cols`: column blocks index the extended row space of the slot's partition. `hub_ids`: distinct vertex ids; vertex v belongs to partition v // 2048; no partition owns more than 48 hubs, and some partition owns exactly 48.
All inputs are finite; a program needn't handle non-finite values.
Results may differ from the reference program's by a relative error of at most 0.0044.
Values may be sent and summed in bfloat16 or wider, within the bound.
No kernel may reach another device: no remote copies, remote signals or barrier semaphores. Data moves between devices by JAX's collectives and lax.ppermute only.
A program may use at most 64 MiB of HBM per device.

```python
import jax
import jax.numpy as jnp
from jax import lax

F_IN = 608
HID = 256
BLK = 128
VDEV = 2048
REACH = 4
HUB_MOST = 48
TILE_MOST = 108
HALO = 1024
HUBS = 256
EXT = 10496
VERTICES = 32768
PARTITIONS = 16
TILES = 1728
N_DOM = 16


def draw_tile_count(key, part):
    lowest = 2 * REACH + 2
    spread = TILE_MOST - lowest + 1
    key_list = jax.random.split(jax.random.fold_in(key, 11), 2)
    raw_draws = jax.random.randint(key_list[0], (N_DOM,), 0, spread)
    counts = lowest + raw_draws * raw_draws // spread
    fullest = jax.random.randint(key_list[1], (), 0, N_DOM)
    counts = jnp.where(jnp.arange(N_DOM) == fullest, TILE_MOST, counts)
    return counts.astype(jnp.int32)


def draw_tile_cols(key, part):
    block_total = ((1 + REACH) * VDEV + HUBS) // BLK
    hub_first = (1 + REACH) * VDEV // BLK
    key_list = jax.random.split(jax.random.fold_in(key, 23), 3)
    columns = jax.random.randint(key_list[0], (N_DOM, TILE_MOST), 0, block_total)
    position = jnp.arange(TILE_MOST)[None, :]
    segment_start = (VDEV + position * (VDEV // 2)) // BLK
    hub_pick = jax.random.randint(key_list[1], (N_DOM, 1), hub_first, block_total)
    local_pick = jax.random.randint(key_list[2], (N_DOM, 1), 0, VDEV // BLK)
    columns = jnp.where(position < 2 * REACH, segment_start, columns)
    columns = jnp.where(position == 2 * REACH, hub_pick, columns)
    columns = jnp.where(position == 2 * REACH + 1, local_pick, columns)
    return columns.reshape(N_DOM * TILE_MOST).astype(jnp.int32)


def draw_hub_ids(key, part):
    key_list = jax.random.split(jax.random.fold_in(key, 37), 4)
    slot_total = N_DOM * HUB_MOST
    positions = jnp.arange(slot_total)
    owners = positions // HUB_MOST
    ranks = positions % HUB_MOST
    device_level = jax.random.randint(key_list[0], (N_DOM,), 0, 4)
    fullest = jax.random.randint(key_list[1], (), 0, N_DOM)
    jitter = jax.random.randint(key_list[2], (slot_total,), 0, 1024)
    scores = (device_level[owners] * 1024 + jitter) * slot_total + positions
    scores = jnp.where(owners == fullest, scores + 8 * 1024 * slot_total, scores)
    chosen = jax.lax.top_k(scores.astype(jnp.int32), HUBS)[1]
    stride = VDEV // HUB_MOST
    shifts = jax.random.randint(key_list[3], (N_DOM,), 0, stride)
    chosen_owner = owners[chosen]
    local_rows = ranks[chosen] * stride + shifts[chosen_owner]
    return (chosen_owner * VDEV + local_rows).astype(jnp.int32)


def with_ends(drawn, own_key, smallest, largest):
    longest = drawn.shape.index(max(drawn.shape))
    spots = []
    for shift in (0, 1):
        where = [jax.random.randint(jax.random.fold_in(own_key, axis), (), 0, length) for axis, length in enumerate(drawn.shape)]
        where[longest] = (where[longest] + shift) % drawn.shape[longest]
        spots.append(tuple(where))
    return drawn.at[spots[0]].set(smallest).at[spots[1]].set(largest)


def block_levels(own_key, shape, cuts, low, top_value):
    level, own = 1.0, jax.random.fold_in(own_key, 6)
    for dim, blocks in cuts:
        draws = jnp.exp(jax.random.uniform(jax.random.fold_in(own, dim), (blocks,), jnp.float32, low / len(cuts), top_value / len(cuts)))
        level = level * jnp.repeat(draws, shape[dim] // blocks).reshape([-1 if axis == dim else 1 for axis in range(len(shape))])
    return level


def bell_draw(rng, extent, scale, bound, cuts=(), kind=jnp.bfloat16):
    values = jax.random.normal(rng, extent, jnp.float32) * scale
    if len(cuts) > 0:
        values = block_levels(rng, extent, cuts, -0.22, 0.18) * values
    return jnp.clip(values, min=-bound, max=bound).astype(kind)


def setup_inputs(seed: int = 0) -> dict:
    seeds = jax.random.split(jax.random.key(seed), 10)
    features = bell_draw(seeds[0], (VERTICES, F_IN), 1.0, 6.0, ((0, 16), (1, 2)))
    weight = bell_draw(seeds[1], (F_IN, HID), F_IN ** -0.5, 0.25)
    out_bias = bell_draw(seeds[2], (HID,), 0.5, 3.0, ((0, 2),), jnp.float32)
    tile_values = bell_draw(seeds[3], (TILES, BLK, BLK), (4 * BLK) ** -0.5, 0.25, ((0, 16),))
    tile_rows = with_ends(jax.random.randint(seeds[4], (TILES,), 0, VDEV // BLK), jax.random.fold_in(seeds[4], 1), 0, (VDEV // BLK) - 1).astype(jnp.int32)
    tile_cols = draw_tile_cols(jax.random.fold_in(seeds[9], 71), 0)
    tile_count = draw_tile_count(jax.random.fold_in(seeds[9], 71), 0)
    send_rows = with_ends(jax.random.randint(seeds[7], (PARTITIONS, 2 * REACH, HALO), 0, VDEV), jax.random.fold_in(seeds[7], 1), 0, VDEV - 1).astype(jnp.int32)
    hub_ids = draw_hub_ids(jax.random.fold_in(seeds[9], 71), 0)
    return {"features": features, "weight": weight, "out_bias": out_bias, "tile_values": tile_values, "tile_rows": tile_rows, "tile_cols": tile_cols, "tile_count": tile_count, "send_rows": send_rows, "hub_ids": hub_ids}


def reference(features, weight, out_bias, tile_values, tile_rows, tile_cols, tile_count, send_rows, hub_ids):
    projected = jnp.dot(features, weight, preferred_element_type=jnp.float32).astype(jnp.bfloat16)
    hub_rows = projected[hub_ids]
    offsets = jnp.array(list(range(-REACH, 0)) + list(range(1, REACH + 1)), jnp.int32)
    slot_ids = jnp.arange(2 * REACH).astype(jnp.int32)

    def one_partition(partition):
        own_rows = lax.dynamic_slice_in_dim(projected, partition * VDEV, VDEV, 0)
        sources = partition - offsets
        present = (sources >= 0) & (sources < N_DOM)
        clipped = jnp.clip(sources, 0, N_DOM - 1).astype(jnp.int32)
        listed = send_rows[clipped, slot_ids]
        picked = projected[clipped[:, None] * VDEV + listed]
        picked = jnp.where(present[:, None, None], picked, jnp.zeros_like(picked))
        extended = jnp.concatenate([own_rows, picked.reshape(REACH * VDEV, HID), hub_rows], 0)
        blocks = extended.reshape(EXT // BLK, BLK, HID)
        col_blocks = lax.dynamic_slice_in_dim(tile_cols, partition * TILE_MOST, TILE_MOST, 0)
        row_blocks = lax.dynamic_slice_in_dim(tile_rows, partition * TILE_MOST, TILE_MOST, 0)
        own_tiles = lax.dynamic_slice_in_dim(tile_values, partition * TILE_MOST, TILE_MOST, 0)
        products = jnp.einsum("tij,tjc->tic", own_tiles.astype(jnp.float32), blocks[col_blocks].astype(jnp.float32), precision=lax.Precision.HIGHEST)
        live_mask = jnp.arange(TILE_MOST).astype(jnp.int32) < tile_count[partition]
        products = jnp.where(live_mask[:, None, None], products, jnp.zeros_like(products))
        aggregate = jax.ops.segment_sum(products, row_blocks, num_segments=VDEV // BLK)
        return jnp.maximum(aggregate.reshape(VDEV, HID) + out_bias, 0.0).astype(jnp.bfloat16)

    result = lax.map(one_partition, jnp.arange(N_DOM, dtype=jnp.int32))
    return result.reshape(N_DOM * VDEV, HID)
```

```python
import functools

import jax
import jax.numpy as jnp
from jax import lax
from jax.experimental import pallas as pl
from jax.experimental.pallas import tpu as pltpu
from jax.sharding import PartitionSpec as P


UNROLL = 4
GATHER_UNROLL = 32


def passed_along(value, axis, steps):
    count = lax.axis_size(axis)
    initial, last = (max(0, -steps), min(count, count - steps))
    return lax.ppermute(value, axis, [(source, source + steps) for source in range(initial, last)])


def summed_over(value, axis):
    count = lax.axis_size(axis)
    if count & (count - 1):
        return lax.psum(value.astype(jnp.float32), axis).astype(value.dtype)
    step = 1
    while step < count:
        value = value + lax.ppermute(value, axis, [(i, i ^ step) for i in range(count)])
        step *= 2
    return value


def project_kernel(local_hubs, *refs, parts):
    features = refs[:parts]
    weights = refs[parts : 2 * parts]
    rows_f32, rows_bf16, hub_part = refs[2 * parts :]
    total = None
    for feature, weight in zip(features, weights):
        piece = lax.dot_general(
            weight[...], feature[...], (((0,), (0,)), ((), ())), preferred_element_type=jnp.float32
        )
        total = piece if total is None else total + piece
    rounded = total.T.astype(jnp.bfloat16)
    rows_bf16[...] = rounded
    rows_f32[...] = rounded.astype(jnp.float32)
    chunk = 256
    ids = local_hubs[...]
    picked = jnp.zeros(hub_part.shape, jnp.float32)
    for start in range(0, rounded.shape[0], chunk):
        lanes = lax.broadcasted_iota(jnp.int32, (ids.shape[0], chunk), 1) + start
        chosen = jnp.where(ids == lanes, 1.0, 0.0).astype(jnp.bfloat16)
        picked += jnp.dot(
            chosen, rounded[start : start + chunk], preferred_element_type=jnp.float32
        )
    hub_part[...] = picked.astype(jnp.bfloat16)


def gather_kernel(send_rows, rows_f32, *refs, slots):
    outs, staged = refs[:-1], refs[-1]
    half = staged.shape[0]
    for slot, out in zip(slots, outs):

        @pl.loop(0, half // GATHER_UNROLL)
        def _(group):
            base = pl.multiple_of(group * GATHER_UNROLL, GATHER_UNROLL)
            for j in range(GATHER_UNROLL):
                row = send_rows[slot, base + j]
                staged[pl.ds(base + j, 1), :] = rows_f32[pl.ds(row, 1), :]

        out[...] = staged[...].astype(jnp.bfloat16)


def listed(rows, cols, count, chosen, first, last, spare):
    chosen_slot, chosen_row, chosen_col = chosen

    def step(t, n):
        col = cols[t]
        chosen_slot[n] = t
        chosen_row[n] = rows[t]
        chosen_col[n] = col
        return n + jnp.where((col >= first) & (col < last), 1, 0)

    n = lax.fori_loop(0, count[0], step, jnp.int32(0))
    for j in range(UNROLL):
        chosen_slot[n + j] = 0
        chosen_row[n + j] = spare
        chosen_col[n + j] = first
    return n


def add_products(n, chosen, tiles, ext, base, acc):
    chosen_slot, chosen_row, chosen_col = chosen
    edge = tiles.shape[1]

    @pl.loop(0, (n + UNROLL - 1) // UNROLL)
    def _(group):
        products = []
        for j in range(UNROLL):
            k = group * UNROLL + j
            start = pl.multiple_of((chosen_col[k] - base) * edge, edge)
            products.append(
                jnp.dot(
                    tiles[chosen_slot[k]],
                    ext[pl.ds(start, edge), :],
                    preferred_element_type=jnp.float32,
                )
            )
        for j in range(UNROLL):
            row = chosen_row[group * UNROLL + j]
            acc[row] += products[j]


def own_kernel(rows, cols, count, tiles, own, acc, *chosen):
    blocks = acc.shape[0] - 1
    acc[...] = jnp.zeros(acc.shape, jnp.float32)
    n = listed(rows, cols, count, chosen, 0, own.shape[0] // tiles.shape[1], blocks)
    add_products(n, chosen, tiles, own, 0, acc)


def rest_kernel(rows, cols, count, bias, tiles, acc_in, *refs):
    sources = refs[:-7]
    out, ext, acc, sems = refs[-7:-3]
    chosen = refs[-3:]
    edge = tiles.shape[1]
    copies, start = [], 0
    for k, source in enumerate(sources):
        copies.append(
            pltpu.make_async_copy(source, ext.at[pl.ds(start, source.shape[0]), :], sems.at[k])
        )
        start += source.shape[0]
        copies[-1].start()
    blocks = acc.shape[0] - 1
    first = blocks
    acc[...] = acc_in[...]
    n = listed(rows, cols, count, chosen, first, first + start // edge, blocks)
    for copy in copies:
        copy.wait()
    add_products(n, chosen, tiles, ext, first, acc)
    total = acc[:blocks].reshape(out.shape)
    out[...] = jnp.maximum(total + bias[...], 0.0).astype(jnp.bfloat16)


def local(
    features, weight, out_bias, tile_values, tile_rows, tile_cols, tile_count, send_rows, hub_ids
):
    column_count = out_bias.shape[0]
    vertex_rows, feature_count = features.shape
    part_index = lax.axis_index("dom")
    feat_index = lax.axis_index("feat")
    feat_size = lax.axis_size("feat")
    slot_total, half_rows = send_rows.shape[1:]
    reach = slot_total // 2
    offsets = list(range(-reach, 0)) + list(range(1, reach + 1))
    edge = tile_values.shape[1]
    blocks = vertex_rows // edge
    hub_total = hub_ids.shape[0]
    smem = pl.BlockSpec(memory_space=pltpu.SMEM)
    vmem = pl.BlockSpec(memory_space=pltpu.VMEM)
    hbm = pl.BlockSpec(memory_space=pl.ANY)

    turned = features.T
    feature_parts, weight_parts = [], []
    for shift in range(feat_size):
        piece = turned
        if shift:
            ring = [(i, (i + shift) % feat_size) for i in range(feat_size)]
            piece = lax.ppermute(turned, "feat", ring)
        origin = (feat_index - shift) % feat_size
        feature_parts.append(piece)
        weight_parts.append(
            lax.dynamic_slice(
                weight,
                (origin * feature_count, feat_index * column_count),
                (feature_count, column_count),
            )
        )
    local_hubs = (hub_ids - part_index * vertex_rows).reshape(hub_total, 1)
    rows_f32, rows_bf16, hub_part = pl.pallas_call(
        functools.partial(project_kernel, parts=feat_size),
        out_shape=(
            jax.ShapeDtypeStruct((vertex_rows, column_count), jnp.float32),
            jax.ShapeDtypeStruct((vertex_rows, column_count), jnp.bfloat16),
            jax.ShapeDtypeStruct((hub_total, column_count), jnp.bfloat16),
        ),
        in_specs=[vmem] * (1 + 2 * feat_size),
        out_specs=[vmem] * 3,
        name="project",
    )(local_hubs, *feature_parts, *weight_parts)
    hub_block = summed_over(hub_part, "dom")

    received = [None] * slot_total
    for far in range(reach):
        slots = (far, slot_total - 1 - far)
        packed = pl.pallas_call(
            functools.partial(gather_kernel, slots=slots),
            out_shape=[jax.ShapeDtypeStruct((half_rows, column_count), jnp.bfloat16)] * 2,
            in_specs=[smem, vmem],
            out_specs=[vmem] * 2,
            scratch_shapes=[pltpu.VMEM((half_rows, column_count), jnp.float32)],
            name="pick_rows",
        )(send_rows[0], rows_f32)
        for slot, rows in zip(slots, packed):
            received[slot] = passed_along(rows, "dom", offsets[slot])

    lists = [pltpu.SMEM((tile_values.shape[0] + UNROLL,), jnp.int32)] * 3
    acc_shape = (blocks + 1, edge, column_count)
    partial_sum = pl.pallas_call(
        own_kernel,
        out_shape=jax.ShapeDtypeStruct(acc_shape, jnp.float32),
        in_specs=[smem] * 3 + [vmem] * 2,
        out_specs=vmem,
        scratch_shapes=lists,
        name="own_tiles",
    )(tile_rows, tile_cols, tile_count, tile_values, rows_bf16)
    sources = received + [hub_block]
    ext_rows = sum(source.shape[0] for source in sources)
    return pl.pallas_call(
        rest_kernel,
        out_shape=jax.ShapeDtypeStruct((vertex_rows, column_count), jnp.bfloat16),
        in_specs=[smem] * 3 + [vmem] * 3 + [hbm] * len(sources),
        out_specs=vmem,
        scratch_shapes=[
            pltpu.VMEM((ext_rows, column_count), jnp.bfloat16),
            pltpu.VMEM(acc_shape, jnp.float32),
            pltpu.SemaphoreType.DMA((len(sources),)),
        ]
        + lists,
        name="other_tiles",
    )(
        tile_rows,
        tile_cols,
        tile_count,
        out_bias.reshape(1, column_count),
        tile_values,
        partial_sum,
        *sources,
    )


def solution(mesh):
    in_specs = (
        P("dom", "feat"),
        P(),
        P("feat"),
        P("dom", None, None),
        P("dom"),
        P("dom"),
        P("dom"),
        P("dom", None, None),
        P(),
    )
    out_specs = P("dom", "feat")
    return jax.shard_map(local, mesh=mesh, in_specs=in_specs, out_specs=out_specs, check_vma=False)
```

```python
import functools

import jax
import jax.numpy as jnp
from jax import lax
from jax.experimental import pallas as pl
from jax.experimental.pallas import tpu as pltpu
from jax.sharding import PartitionSpec as P


UNROLL = 4
FOLDS = 4
ORDER = ((5, 4), (2, 3), (6, 7), (1, 0))


def passed_along(value, axis, steps):
    count = lax.axis_size(axis)
    initial, last = (max(0, -steps), min(count, count - steps))
    return lax.ppermute(value, axis, [(source, source + steps) for source in range(initial, last)])


def exchanged(value, axis, step):
    count = lax.axis_size(axis)
    return lax.ppermute(value, axis, [(i, i ^ step) for i in range(count)])


def send_order(reach):
    if reach == 4:
        return ORDER
    return tuple((k, 2 * reach - 1 - k) for k in range(reach))


def project_kernel(local_hubs, *refs, parts):
    features = refs[:parts]
    weights = refs[parts : 2 * parts]
    folded, rows_bf16, hub_part = refs[2 * parts :]
    total = None
    for feature, weight in zip(features, weights):
        piece = lax.dot_general(
            weight[...], feature[...], (((0,), (0,)), ((), ())), preferred_element_type=jnp.float32
        )
        total = piece if total is None else total + piece
    rounded = total.T.astype(jnp.bfloat16)
    rows_bf16[...] = rounded
    depth, width = folded.shape[0], rounded.shape[1]
    for k in range(folded.shape[1] // width):
        folded[:, k * width : (k + 1) * width] = rounded[k * depth : (k + 1) * depth]
    chunk = 256
    ids = local_hubs[...]
    picked = jnp.zeros(hub_part.shape, jnp.float32)
    for start in range(0, rounded.shape[0], chunk):
        lanes = lax.broadcasted_iota(jnp.int32, (ids.shape[0], chunk), 1) + start
        chosen = jnp.where(ids == lanes, 1.0, 0.0).astype(jnp.bfloat16)
        picked += jnp.dot(
            chosen, rounded[start : start + chunk], preferred_element_type=jnp.float32
        )
    hub_part[...] = picked.astype(jnp.bfloat16)


def pick_kernel(send_rows, folded, *refs, slots, with_hubs):
    outs = refs[-len(slots) :]
    if with_hubs:
        mine, theirs, summed = refs[:3]
        summed[...] = mine[...] + theirs[...]
    depth, total_width = folded.shape
    source = folded[...]
    turned = send_rows[...].T
    piece = 256
    for slot, out in zip(slots, outs):
        width = out.shape[1]
        for start in range(0, out.shape[0], piece):
            ids = turned[start : start + piece, slot : slot + 1]
            lanes = lax.broadcasted_iota(jnp.int32, (piece, depth), 1)
            chosen = jnp.where((ids & (depth - 1)) == lanes, 1.0, 0.0).astype(jnp.bfloat16)
            wide = jnp.dot(chosen, source, preferred_element_type=jnp.float32)
            picked = wide[:, :width]
            for k in range(1, total_width // width):
                picked = jnp.where(ids >= k * depth, wide[:, k * width : (k + 1) * width], picked)
            out[start : start + piece] = picked.astype(jnp.bfloat16)


def listed(rows, cols, count, chosen, first, last, spare):
    chosen_slot, chosen_row, chosen_col = chosen

    def step(t, n):
        col = cols[t]
        chosen_slot[n] = t
        chosen_row[n] = rows[t]
        chosen_col[n] = col
        return n + jnp.where((col >= first) & (col < last), 1, 0)

    n = lax.fori_loop(0, count[0], step, jnp.int32(0))
    for j in range(UNROLL):
        chosen_slot[n + j] = 0
        chosen_row[n + j] = spare
        chosen_col[n + j] = first
    return n


def add_products(n, chosen, tiles, ext, base, acc):
    chosen_slot, chosen_row, chosen_col = chosen
    edge = tiles.shape[1]

    @pl.loop(0, (n + UNROLL - 1) // UNROLL)
    def _(group):
        products = []
        for j in range(UNROLL):
            k = group * UNROLL + j
            start = pl.multiple_of((chosen_col[k] - base) * edge, edge)
            products.append(
                jnp.dot(
                    tiles[chosen_slot[k]],
                    ext[pl.ds(start, edge), :],
                    preferred_element_type=jnp.float32,
                )
            )
        for j in range(UNROLL):
            row = chosen_row[group * UNROLL + j]
            acc[row] += products[j]


def own_kernel(rows, cols, count, tiles, own, acc, *chosen):
    blocks = acc.shape[0] - 1
    acc[...] = jnp.zeros(acc.shape, jnp.float32)
    n = listed(rows, cols, count, chosen, 0, own.shape[0] // tiles.shape[1], blocks)
    add_products(n, chosen, tiles, own, 0, acc)


def rest_kernel(rows, cols, count, bias, tiles, acc_in, *refs):
    sources = refs[:-7]
    out, ext, acc, sems = refs[-7:-3]
    chosen = refs[-3:]
    edge = tiles.shape[1]
    copies, start = [], 0
    for k, source in enumerate(sources):
        copies.append(
            pltpu.make_async_copy(source, ext.at[pl.ds(start, source.shape[0]), :], sems.at[k])
        )
        start += source.shape[0]
        copies[-1].start()
    blocks = acc.shape[0] - 1
    first = blocks
    acc[...] = acc_in[...]
    n = listed(rows, cols, count, chosen, first, first + start // edge, blocks)
    for copy in copies:
        copy.wait()
    add_products(n, chosen, tiles, ext, first, acc)
    total = acc[:blocks].reshape(out.shape)
    out[...] = jnp.maximum(total + bias[...], 0.0).astype(jnp.bfloat16)


def local(
    features, weight, out_bias, tile_values, tile_rows, tile_cols, tile_count, send_rows, hub_ids
):
    column_count = out_bias.shape[0]
    vertex_rows, feature_count = features.shape
    part_index = lax.axis_index("dom")
    feat_index = lax.axis_index("feat")
    feat_size = lax.axis_size("feat")
    part_count = lax.axis_size("dom")
    slot_total, half_rows = send_rows.shape[1:]
    reach = slot_total // 2
    offsets = list(range(-reach, 0)) + list(range(1, reach + 1))
    edge = tile_values.shape[1]
    blocks = vertex_rows // edge
    hub_total = hub_ids.shape[0]
    smem = pl.BlockSpec(memory_space=pltpu.SMEM)
    vmem = pl.BlockSpec(memory_space=pltpu.VMEM)
    hbm = pl.BlockSpec(memory_space=pl.ANY)

    turned = features.T
    feature_parts, weight_parts = [], []
    for shift in range(feat_size):
        piece = turned
        if shift:
            ring = [(i, (i + shift) % feat_size) for i in range(feat_size)]
            piece = lax.ppermute(turned, "feat", ring)
        origin = (feat_index - shift) % feat_size
        feature_parts.append(piece)
        weight_parts.append(
            lax.dynamic_slice(
                weight,
                (origin * feature_count, feat_index * column_count),
                (feature_count, column_count),
            )
        )
    local_hubs = (hub_ids - part_index * vertex_rows).reshape(hub_total, 1)
    folds = FOLDS if column_count % 128 == 0 else 1
    depth = vertex_rows // folds
    assert depth & (depth - 1) == 0
    folded, rows_bf16, hub_part = pl.pallas_call(
        functools.partial(project_kernel, parts=feat_size),
        out_shape=(
            jax.ShapeDtypeStruct((depth, folds * column_count), jnp.bfloat16),
            jax.ShapeDtypeStruct((vertex_rows, column_count), jnp.bfloat16),
            jax.ShapeDtypeStruct((hub_total, column_count), jnp.bfloat16),
        ),
        in_specs=[vmem] * (1 + 2 * feat_size),
        out_specs=[vmem] * 3,
        name="project",
    )(local_hubs, *feature_parts, *weight_parts)
    steps = []
    while 1 << len(steps) < part_count:
        steps.append(1 << len(steps))
    assert part_count == 1 << len(steps)
    hub_mine, hub_theirs, stage = hub_part, None, 0

    def start_stage():
        nonlocal hub_theirs, stage
        if stage < len(steps):
            hub_theirs = exchanged(hub_mine, "dom", steps[stage])
            stage += 1
        else:
            hub_theirs = None

    start_stage()
    received = [None] * slot_total
    row_type = jax.ShapeDtypeStruct((half_rows, column_count), jnp.bfloat16)
    hub_type = jax.ShapeDtypeStruct((hub_total, column_count), jnp.bfloat16)
    for group, slots in enumerate(send_order(reach)):
        hubs = group > 0 and hub_theirs is not None
        picked = pl.pallas_call(
            functools.partial(pick_kernel, slots=slots, with_hubs=hubs),
            out_shape=[hub_type] * hubs + [row_type] * len(slots),
            in_specs=[vmem] * (2 + 2 * hubs),
            out_specs=[vmem] * (hubs + len(slots)),
            name="pick_rows",
        )(send_rows[0], folded, *([hub_mine, hub_theirs] if hubs else []))
        if hubs:
            hub_mine = picked[0]
            start_stage()
        for slot, rows in zip(slots, picked[hubs:]):
            received[slot] = passed_along(rows, "dom", offsets[slot])
    while hub_theirs is not None:
        hub_mine = hub_mine + hub_theirs
        start_stage()
    hub_block = hub_mine

    lists = [pltpu.SMEM((tile_values.shape[0] + UNROLL,), jnp.int32)] * 3
    acc_shape = (blocks + 1, edge, column_count)
    partial_sum = pl.pallas_call(
        own_kernel,
        out_shape=jax.ShapeDtypeStruct(acc_shape, jnp.float32),
        in_specs=[smem] * 3 + [vmem] * 2,
        out_specs=vmem,
        scratch_shapes=lists,
        name="own_tiles",
    )(tile_rows, tile_cols, tile_count, tile_values, rows_bf16)
    sources = received + [hub_block]
    ext_rows = sum(source.shape[0] for source in sources)
    return pl.pallas_call(
        rest_kernel,
        out_shape=jax.ShapeDtypeStruct((vertex_rows, column_count), jnp.bfloat16),
        in_specs=[smem] * 3 + [vmem] * 3 + [hbm] * len(sources),
        out_specs=vmem,
        scratch_shapes=[
            pltpu.VMEM((ext_rows, column_count), jnp.bfloat16),
            pltpu.VMEM(acc_shape, jnp.float32),
            pltpu.SemaphoreType.DMA((len(sources),)),
        ]
        + lists,
        name="other_tiles",
    )(
        tile_rows,
        tile_cols,
        tile_count,
        out_bias.reshape(1, column_count),
        tile_values,
        partial_sum,
        *sources,
    )


def solution(mesh):
    in_specs = (
        P("dom", "feat"),
        P(),
        P("feat"),
        P("dom", None, None),
        P("dom"),
        P("dom"),
        P("dom"),
        P("dom", None, None),
        P(),
    )
    out_specs = P("dom", "feat")
    return jax.shard_map(local, mesh=mesh, in_specs=in_specs, out_specs=out_specs, check_vma=False)
```

```python
import functools

import jax
import jax.numpy as jnp
from jax import lax
from jax.experimental import pallas as pl
from jax.experimental.pallas import tpu as pltpu
from jax.sharding import PartitionSpec as P


UNROLL = 4
FOLDS = 4
ORDER = ((5, 4), (2, 3), (6, 7), (1, 0))


def passed_along(value, axis, steps):
    count = lax.axis_size(axis)
    initial, last = (max(0, -steps), min(count, count - steps))
    return lax.ppermute(value, axis, [(source, source + steps) for source in range(initial, last)])


def exchanged(value, axis, step):
    count = lax.axis_size(axis)
    return lax.ppermute(value, axis, [(i, i ^ step) for i in range(count)])


def send_order(reach):
    if reach == 4:
        return ORDER
    return tuple((reach + k, reach - 1 - k) for k in range(reach))


def project_kernel(local_hubs, *refs, parts):
    features = refs[:parts]
    weights = refs[parts : 2 * parts]
    folded, rows_bf16, hub_part = refs[2 * parts :]
    total = None
    for feature, weight in zip(features, weights):
        piece = lax.dot_general(
            weight[...], feature[...], (((0,), (0,)), ((), ())), preferred_element_type=jnp.float32
        )
        total = piece if total is None else total + piece
    rounded = total.T.astype(jnp.bfloat16)
    rows_bf16[...] = rounded
    depth, width = folded.shape[0], rounded.shape[1]
    for k in range(folded.shape[1] // width):
        folded[:, k * width : (k + 1) * width] = rounded[k * depth : (k + 1) * depth]
    chunk = 256
    ids = local_hubs[...]
    picked = jnp.zeros(hub_part.shape, jnp.float32)
    for start in range(0, rounded.shape[0], chunk):
        lanes = lax.broadcasted_iota(jnp.int32, (ids.shape[0], chunk), 1) + start
        chosen = jnp.where(ids == lanes, 1.0, 0.0).astype(jnp.bfloat16)
        picked += jnp.dot(
            chosen, rounded[start : start + chunk], preferred_element_type=jnp.float32
        )
    hub_part[...] = picked.astype(jnp.bfloat16)


def pick_kernel(send_rows, folded, *refs, slots, with_hubs):
    outs = refs[-len(slots) :]
    if with_hubs:
        mine, theirs, summed = refs[:3]
        summed[...] = mine[...] + theirs[...]
    depth, total_width = folded.shape
    source = folded[...]
    turned = send_rows[...].T
    piece = 256
    for slot, out in zip(slots, outs):
        width = out.shape[1]
        for start in range(0, out.shape[0], piece):
            ids = turned[start : start + piece, slot : slot + 1]
            lanes = lax.broadcasted_iota(jnp.int32, (piece, depth), 1)
            chosen = jnp.where((ids & (depth - 1)) == lanes, 1.0, 0.0).astype(jnp.bfloat16)
            wide = jnp.dot(chosen, source, preferred_element_type=jnp.float32)
            picked = wide[:, :width]
            for k in range(1, total_width // width):
                picked = jnp.where(ids >= k * depth, wide[:, k * width : (k + 1) * width], picked)
            out[start : start + piece] = picked.astype(jnp.bfloat16)


def listed(rows, cols, count, chosen, ranges, spare):
    chosen_slot, chosen_row, chosen_col = chosen

    def step(t, n):
        col = cols[t]
        chosen_slot[n] = t
        chosen_row[n] = rows[t]
        chosen_col[n] = col
        inside = jnp.int32(0)
        for first, last in ranges:
            inside += jnp.where((col >= first) & (col < last), 1, 0)
        return n + inside

    n = lax.fori_loop(0, count[0], step, jnp.int32(0))
    for j in range(UNROLL):
        chosen_slot[n + j] = 0
        chosen_row[n + j] = spare
        chosen_col[n + j] = ranges[0][0]
    return n


def add_products(n, chosen, tiles, ext, acc):
    chosen_slot, chosen_row, chosen_col = chosen
    edge = tiles.shape[1]

    @pl.loop(0, (n + UNROLL - 1) // UNROLL)
    def _(group):
        products = []
        for j in range(UNROLL):
            k = group * UNROLL + j
            start = pl.multiple_of(chosen_col[k] * edge, edge)
            products.append(
                jnp.dot(
                    tiles[chosen_slot[k]],
                    ext[pl.ds(start, edge), :],
                    preferred_element_type=jnp.float32,
                )
            )
        for j in range(UNROLL):
            row = chosen_row[group * UNROLL + j]
            acc[row] += products[j]


def own_kernel(rows, cols, count, tiles, own, acc, *chosen):
    blocks = acc.shape[0] - 1
    acc[...] = jnp.zeros(acc.shape, jnp.float32)
    n = listed(rows, cols, count, chosen, ((0, blocks),), blocks)
    add_products(n, chosen, tiles, own, acc)


def more_kernel(rows, cols, count, bias, tiles, acc_in, *refs, starts, finish):
    sources = refs[: len(starts)]
    refs = refs[len(starts) :]
    if finish:
        out, ext, sems, acc = refs[:4]
    else:
        acc, ext, sems = refs[:3]
    chosen = refs[-3:]
    edge = tiles.shape[1]
    copies, ranges = [], []
    for k, (source, start) in enumerate(zip(sources, starts)):
        length = source.shape[0]
        copies.append(
            pltpu.make_async_copy(source, ext.at[pl.ds(start, length), :], sems.at[k])
        )
        copies[-1].start()
        first, last = start // edge, (start + length) // edge
        if ranges and ranges[-1][1] == first:
            ranges[-1] = (ranges[-1][0], last)
        else:
            ranges.append((first, last))
    blocks = acc.shape[0] - 1
    acc[...] = acc_in[...]
    n = listed(rows, cols, count, chosen, ranges, blocks)
    for copy in copies:
        copy.wait()
    add_products(n, chosen, tiles, ext, acc)
    if finish:
        total = acc[:blocks].reshape(out.shape)
        out[...] = jnp.maximum(total + bias[...], 0.0).astype(jnp.bfloat16)


def local(
    features, weight, out_bias, tile_values, tile_rows, tile_cols, tile_count, send_rows, hub_ids
):
    column_count = out_bias.shape[0]
    vertex_rows, feature_count = features.shape
    part_index = lax.axis_index("dom")
    feat_index = lax.axis_index("feat")
    feat_size = lax.axis_size("feat")
    part_count = lax.axis_size("dom")
    slot_total, half_rows = send_rows.shape[1:]
    reach = slot_total // 2
    offsets = list(range(-reach, 0)) + list(range(1, reach + 1))
    edge = tile_values.shape[1]
    blocks = vertex_rows // edge
    hub_total = hub_ids.shape[0]
    smem = pl.BlockSpec(memory_space=pltpu.SMEM)
    vmem = pl.BlockSpec(memory_space=pltpu.VMEM)
    hbm = pl.BlockSpec(memory_space=pl.ANY)

    turned = features.T
    feature_parts, weight_parts = [], []
    for shift in range(feat_size):
        piece = turned
        if shift:
            ring = [(i, (i + shift) % feat_size) for i in range(feat_size)]
            piece = lax.ppermute(turned, "feat", ring)
        origin = (feat_index - shift) % feat_size
        feature_parts.append(piece)
        weight_parts.append(
            lax.dynamic_slice(
                weight,
                (origin * feature_count, feat_index * column_count),
                (feature_count, column_count),
            )
        )
    local_hubs = (hub_ids - part_index * vertex_rows).reshape(hub_total, 1)
    folds = FOLDS if column_count % 128 == 0 else 1
    depth = vertex_rows // folds
    assert depth & (depth - 1) == 0
    folded, rows_bf16, hub_part = pl.pallas_call(
        functools.partial(project_kernel, parts=feat_size),
        out_shape=(
            jax.ShapeDtypeStruct((depth, folds * column_count), jnp.bfloat16),
            jax.ShapeDtypeStruct((vertex_rows, column_count), jnp.bfloat16),
            jax.ShapeDtypeStruct((hub_total, column_count), jnp.bfloat16),
        ),
        in_specs=[vmem] * (1 + 2 * feat_size),
        out_specs=[vmem] * 3,
        name="project",
    )(local_hubs, *feature_parts, *weight_parts)
    steps = []
    while 1 << len(steps) < part_count:
        steps.append(1 << len(steps))
    assert part_count == 1 << len(steps)
    hub_mine, hub_theirs, stage = hub_part, None, 0

    def start_stage():
        nonlocal hub_theirs, stage
        if stage < len(steps):
            hub_theirs = exchanged(hub_mine, "dom", steps[stage])
            stage += 1
        else:
            hub_theirs = None

    start_stage()
    received = [None] * slot_total
    row_type = jax.ShapeDtypeStruct((half_rows, column_count), jnp.bfloat16)
    hub_type = jax.ShapeDtypeStruct((hub_total, column_count), jnp.bfloat16)
    for group, slots in enumerate(send_order(reach)):
        hubs = group % 2 == 1 and hub_theirs is not None
        picked = pl.pallas_call(
            functools.partial(pick_kernel, slots=slots, with_hubs=hubs),
            out_shape=[hub_type] * hubs + [row_type] * len(slots),
            in_specs=[vmem] * (2 + 2 * hubs),
            out_specs=[vmem] * (hubs + len(slots)),
            name="pick_rows",
        )(send_rows[0], folded, *([hub_mine, hub_theirs] if hubs else []))
        if hubs:
            hub_mine = picked[0]
            start_stage()
        for slot, rows in zip(slots, picked[hubs:]):
            received[slot] = passed_along(rows, "dom", offsets[slot])
    lists = [pltpu.SMEM((tile_values.shape[0] + UNROLL,), jnp.int32)] * 3
    acc_shape = (blocks + 1, edge, column_count)
    partial_sum = pl.pallas_call(
        own_kernel,
        out_shape=jax.ShapeDtypeStruct(acc_shape, jnp.float32),
        in_specs=[smem] * 3 + [vmem] * 2,
        out_specs=vmem,
        scratch_shapes=lists,
        name="own_tiles",
    )(tile_rows, tile_cols, tile_count, tile_values, rows_bf16)
    while hub_theirs is not None:
        hub_mine = hub_mine + hub_theirs
        start_stage()

    ext_rows = vertex_rows + slot_total * half_rows + hub_total

    def add_more(held, arrays, finish):
        starts = [vertex_rows + slot * half_rows for slot in held]
        scratch = [
            pltpu.VMEM((ext_rows, column_count), jnp.bfloat16),
            pltpu.SemaphoreType.DMA((len(held),)),
        ]
        if finish:
            shape = jax.ShapeDtypeStruct((vertex_rows, column_count), jnp.bfloat16)
            scratch.append(pltpu.VMEM(acc_shape, jnp.float32))
        else:
            shape = jax.ShapeDtypeStruct(acc_shape, jnp.float32)
        return pl.pallas_call(
            functools.partial(more_kernel, starts=starts, finish=finish),
            out_shape=shape,
            in_specs=[smem] * 3 + [vmem] * 3 + [hbm] * len(held),
            out_specs=vmem,
            scratch_shapes=scratch + lists,
            name="other_tiles",
        )(
            tile_rows,
            tile_cols,
            tile_count,
            out_bias.reshape(1, column_count),
            tile_values,
            partial_sum,
            *arrays,
        )

    order = [slot for slots in send_order(reach) for slot in slots]
    early, late = sorted(order[:reach]), sorted(order[reach:])
    partial_sum = add_more(early, [received[slot] for slot in early], False)
    return add_more(
        late + [slot_total], [received[slot] for slot in late] + [hub_mine], True
    )


def solution(mesh):
    in_specs = (
        P("dom", "feat"),
        P(),
        P("feat"),
        P("dom", None, None),
        P("dom"),
        P("dom"),
        P("dom"),
        P("dom", None, None),
        P(),
    )
    out_specs = P("dom", "feat")
    return jax.shard_map(local, mesh=mesh, in_specs=in_specs, out_specs=out_specs, check_vma=False)
```

```python
import functools

import jax
import jax.numpy as jnp
from jax import lax
from jax.experimental import pallas as pl
from jax.experimental.pallas import tpu as pltpu
from jax.sharding import PartitionSpec as P


UNROLL = 4
FOLDS = 4
ORDER = ((5, 4, 2, 3), (6, 7, 1, 0))


def passed_along(value, axis, steps):
    count = lax.axis_size(axis)
    initial, last = (max(0, -steps), min(count, count - steps))
    return lax.ppermute(value, axis, [(source, source + steps) for source in range(initial, last)])


def exchanged(value, axis, step):
    count = lax.axis_size(axis)
    return lax.ppermute(value, axis, [(i, i ^ step) for i in range(count)])


def send_order(reach):
    if reach == 4:
        return ORDER
    near = [slot for k in range(reach) for slot in (reach + k, reach - 1 - k)]
    return tuple(near[:reach]), tuple(near[reach:])


def project_kernel(local_hubs, *refs, parts):
    features = refs[:parts]
    weights = refs[parts : 2 * parts]
    folded, rows_bf16, hub_part = refs[2 * parts :]
    total = None
    for feature, weight in zip(features, weights):
        piece = lax.dot_general(
            weight[...], feature[...], (((0,), (0,)), ((), ())), preferred_element_type=jnp.float32
        )
        total = piece if total is None else total + piece
    rounded = total.T.astype(jnp.bfloat16)
    rows_bf16[...] = rounded
    depth, width = folded.shape[0], rounded.shape[1]
    for k in range(folded.shape[1] // width):
        folded[:, k * width : (k + 1) * width] = rounded[k * depth : (k + 1) * depth]
    chunk = 256
    ids = local_hubs[...]
    picked = jnp.zeros(hub_part.shape, jnp.float32)
    for start in range(0, rounded.shape[0], chunk):
        lanes = lax.broadcasted_iota(jnp.int32, (ids.shape[0], chunk), 1) + start
        chosen = jnp.where(ids == lanes, 1.0, 0.0).astype(jnp.bfloat16)
        picked += jnp.dot(
            chosen, rounded[start : start + chunk], preferred_element_type=jnp.float32
        )
    hub_part[...] = picked.astype(jnp.bfloat16)


def pick_kernel(send_rows, folded, *refs, slots, with_hubs):
    outs = refs[-len(slots) :]
    if with_hubs:
        mine, theirs, summed = refs[:3]
        summed[...] = mine[...] + theirs[...]
    depth, total_width = folded.shape
    source = folded[...]
    turned = send_rows[...].T
    piece = 256
    for slot, out in zip(slots, outs):
        width = out.shape[1]
        for start in range(0, out.shape[0], piece):
            ids = turned[start : start + piece, slot : slot + 1]
            lanes = lax.broadcasted_iota(jnp.int32, (piece, depth), 1)
            chosen = jnp.where((ids & (depth - 1)) == lanes, 1.0, 0.0).astype(jnp.bfloat16)
            wide = jnp.dot(chosen, source, preferred_element_type=jnp.float32)
            picked = wide[:, :width]
            for k in range(1, total_width // width):
                picked = jnp.where(ids >= k * depth, wide[:, k * width : (k + 1) * width], picked)
            out[start : start + piece] = picked.astype(jnp.bfloat16)


def fetched(rows, cols, count, tiles, lists, ranges, spare):
    held, sems, chosen_row, chosen_col = lists

    def step(t, n):
        col = cols[t]
        chosen_row[n] = rows[t]
        chosen_col[n] = col
        inside = (col >= ranges[0][0]) & (col < ranges[0][1])
        for first, last in ranges[1:]:
            inside |= (col >= first) & (col < last)

        @pl.when(inside)
        def _():
            pltpu.make_async_copy(tiles.at[t], held.at[n], sems.at[n]).start()

        return n + jnp.where(inside, 1, 0)

    n = lax.fori_loop(0, count[0], step, jnp.int32(0))
    for j in range(UNROLL):
        chosen_row[n + j] = spare
        chosen_col[n + j] = ranges[0][0]
    return n


def add_products(n, tiles, lists, ext, acc):
    held, sems, chosen_row, chosen_col = lists
    edge = held.shape[1]

    @pl.loop(0, (n + UNROLL - 1) // UNROLL)
    def _(group):
        products = []
        for j in range(UNROLL):
            k = group * UNROLL + j

            @pl.when(k < n)
            def _():
                pltpu.make_async_copy(tiles.at[0], held.at[k], sems.at[k]).wait()

        for j in range(UNROLL):
            k = group * UNROLL + j
            start = pl.multiple_of(chosen_col[k] * edge, edge)
            products.append(
                jnp.dot(
                    held[jnp.minimum(k, n - 1)],
                    ext[pl.ds(start, edge), :],
                    preferred_element_type=jnp.float32,
                )
            )
        for j in range(UNROLL):
            row = chosen_row[group * UNROLL + j]
            acc[row] += products[j]


def own_kernel(rows, cols, count, tiles, own, acc, *lists):
    blocks = acc.shape[0] - 1
    n = fetched(rows, cols, count, tiles, lists, ((0, blocks),), blocks)
    acc[...] = jnp.zeros(acc.shape, jnp.float32)
    add_products(n, tiles, lists, own, acc)


def rest_kernel(rows, cols, count, bias, tiles, acc_in, *refs):
    sources = refs[:-8]
    out, ext, acc, source_sems = refs[-8:-4]
    lists = refs[-4:]
    edge = tiles.shape[1]
    blocks = acc.shape[0] - 1
    copies, start = [], blocks * edge
    for k, source in enumerate(sources):
        copies.append(
            pltpu.make_async_copy(
                source, ext.at[pl.ds(start, source.shape[0]), :], source_sems.at[k]
            )
        )
        start += source.shape[0]
        copies[-1].start()
    n = fetched(rows, cols, count, tiles, lists, ((blocks, start // edge),), blocks)
    acc[...] = acc_in[...]
    for copy in copies:
        copy.wait()
    add_products(n, tiles, lists, ext, acc)
    total = acc[:blocks].reshape(out.shape)
    out[...] = jnp.maximum(total + bias[...], 0.0).astype(jnp.bfloat16)


def local(
    features, weight, out_bias, tile_values, tile_rows, tile_cols, tile_count, send_rows, hub_ids
):
    column_count = out_bias.shape[0]
    vertex_rows, feature_count = features.shape
    part_index = lax.axis_index("dom")
    feat_index = lax.axis_index("feat")
    feat_size = lax.axis_size("feat")
    part_count = lax.axis_size("dom")
    slot_total, half_rows = send_rows.shape[1:]
    reach = slot_total // 2
    offsets = list(range(-reach, 0)) + list(range(1, reach + 1))
    edge = tile_values.shape[1]
    blocks = vertex_rows // edge
    hub_total = hub_ids.shape[0]
    smem = pl.BlockSpec(memory_space=pltpu.SMEM)
    vmem = pl.BlockSpec(memory_space=pltpu.VMEM)
    hbm = pl.BlockSpec(memory_space=pl.ANY)

    turned = features.T
    feature_parts, weight_parts = [], []
    for shift in range(feat_size):
        piece = turned
        if shift:
            ring = [(i, (i + shift) % feat_size) for i in range(feat_size)]
            piece = lax.ppermute(turned, "feat", ring)
        origin = (feat_index - shift) % feat_size
        feature_parts.append(piece)
        weight_parts.append(
            lax.dynamic_slice(
                weight,
                (origin * feature_count, feat_index * column_count),
                (feature_count, column_count),
            )
        )
    local_hubs = (hub_ids - part_index * vertex_rows).reshape(hub_total, 1)
    folds = FOLDS if column_count % 128 == 0 else 1
    depth = vertex_rows // folds
    assert depth & (depth - 1) == 0
    folded, rows_bf16, hub_part = pl.pallas_call(
        functools.partial(project_kernel, parts=feat_size),
        out_shape=(
            jax.ShapeDtypeStruct((depth, folds * column_count), jnp.bfloat16),
            jax.ShapeDtypeStruct((vertex_rows, column_count), jnp.bfloat16),
            jax.ShapeDtypeStruct((hub_total, column_count), jnp.bfloat16),
        ),
        in_specs=[vmem] * (1 + 2 * feat_size),
        out_specs=[vmem] * 3,
        name="project",
    )(local_hubs, *feature_parts, *weight_parts)
    steps = []
    while 1 << len(steps) < part_count:
        steps.append(1 << len(steps))
    assert part_count == 1 << len(steps)
    hub_mine, hub_theirs, stage = hub_part, None, 0

    def start_stage():
        nonlocal hub_theirs, stage
        if stage < len(steps):
            hub_theirs = exchanged(hub_mine, "dom", steps[stage])
            stage += 1
        else:
            hub_theirs = None

    start_stage()
    received = [None] * slot_total
    row_type = jax.ShapeDtypeStruct((half_rows, column_count), jnp.bfloat16)
    hub_type = jax.ShapeDtypeStruct((hub_total, column_count), jnp.bfloat16)
    for group, slots in enumerate(send_order(reach)):
        hubs = group % 2 == 1 and hub_theirs is not None
        picked = pl.pallas_call(
            functools.partial(pick_kernel, slots=slots, with_hubs=hubs),
            out_shape=[hub_type] * hubs + [row_type] * len(slots),
            in_specs=[vmem] * (2 + 2 * hubs),
            out_specs=[vmem] * (hubs + len(slots)),
            name="pick_rows",
        )(send_rows[0], folded, *([hub_mine, hub_theirs] if hubs else []))
        if hubs:
            hub_mine = picked[0]
            start_stage()
        for slot, rows in zip(slots, picked[hubs:]):
            received[slot] = passed_along(rows, "dom", offsets[slot])
    tile_slots = tile_values.shape[0]
    lists = [
        pltpu.VMEM(tile_values.shape, tile_values.dtype),
        pltpu.SemaphoreType.DMA((tile_slots,)),
        pltpu.SMEM((tile_slots + UNROLL,), jnp.int32),
        pltpu.SMEM((tile_slots + UNROLL,), jnp.int32),
    ]
    acc_shape = (blocks + 1, edge, column_count)
    partial_sum = pl.pallas_call(
        own_kernel,
        out_shape=jax.ShapeDtypeStruct(acc_shape, jnp.float32),
        in_specs=[smem] * 3 + [hbm, vmem],
        out_specs=vmem,
        scratch_shapes=lists,
        name="own_tiles",
    )(tile_rows, tile_cols, tile_count, tile_values, rows_bf16)
    while hub_theirs is not None:
        hub_mine = hub_mine + hub_theirs
        start_stage()
    sources = received + [hub_mine]
    ext_rows = vertex_rows + sum(source.shape[0] for source in sources)
    return pl.pallas_call(
        rest_kernel,
        out_shape=jax.ShapeDtypeStruct((vertex_rows, column_count), jnp.bfloat16),
        in_specs=[smem] * 3 + [vmem, hbm, vmem] + [hbm] * len(sources),
        out_specs=vmem,
        scratch_shapes=[
            pltpu.VMEM((ext_rows, column_count), jnp.bfloat16),
            pltpu.VMEM(acc_shape, jnp.float32),
            pltpu.SemaphoreType.DMA((len(sources),)),
        ]
        + lists,
        name="other_tiles",
    )(
        tile_rows,
        tile_cols,
        tile_count,
        out_bias.reshape(1, column_count),
        tile_values,
        partial_sum,
        *sources,
    )


def solution(mesh):
    in_specs = (
        P("dom", "feat"),
        P(),
        P("feat"),
        P("dom", None, None),
        P("dom"),
        P("dom"),
        P("dom"),
        P("dom", None, None),
        P(),
    )
    out_specs = P("dom", "feat")
    return jax.shard_map(local, mesh=mesh, in_specs=in_specs, out_specs=out_specs, check_vma=False)
```
